32 devices in a mesh: ctx: 4 (over y, x), head: 8 (over z, core).
Axes of the slice: x: 2, y: 2, z: 4, core: 2. Of those that a mesh axis runs over, the one named last changes fastest.
Arguments:
- queries: bfloat16 [512, 3072], P('ctx', 'head'), may hold values from -10 to 10
- latent: bfloat16 [512, 576], P('ctx'), may hold values from -10 to 10
- block_of: int32 [8], replicated, may hold values from 0 to 7, each once
- key_up: bfloat16 [16, 128, 512], P('head'), may hold values from -0.5 to 0.5
- value_up: bfloat16 [16, 512, 128], P('head'), may hold values from -0.25 to 0.25
- out_grad: bfloat16 [512, 2048], P('ctx', 'head'), may hold values from -6 to 6
Outputs:
- attended: bfloat16 [512, 2048], P('ctx', 'head')
- query_grad: bfloat16 [512, 3072], P('ctx', 'head')
- latent_grad: float32 [512, 576], P('ctx')
The draws below stay inside these ranges and needn't reach their ends.
Inputs may be any that keep to these rules, and one draw needn't show every extreme that they name: `block_of`: a permutation of the 8 blocks.
All inputs are finite; a program needn't handle non-finite values.
Results may differ from the reference program's by a relative error of at most 0.0099.
Values may be sent and summed in bfloat16 or wider, within the bound.
No kernel may reach another device: no remote copies, remote signals or barrier semaphores. Data moves between devices by JAX's collectives and lax.ppermute only.
A program may use at most 64 MiB of HBM per device.

```python
import math
import jax
import jax.numpy as jnp
from jax import lax

LATENT = 512
ROPE = 64
NOPE = 128
VHEAD = 128
HEADS = 16
TOKENS = 512
BLK = 64
BLOCKS = 8


def draw_queries(key, part):
    shape = (TOKENS, HEADS, NOPE + ROPE)
    base = jnp.clip(jax.random.normal(jax.random.fold_in(key, 1), shape, jnp.float32), -6.0, 6.0)
    return base.reshape(TOKENS, HEADS * (NOPE + ROPE)).astype(jnp.bfloat16)


def draw_latent(key, part):
    shape = (TOKENS, LATENT + ROPE)
    base = jnp.clip(jax.random.normal(jax.random.fold_in(key, 3), shape, jnp.float32), -6.0, 6.0)
    return base.astype(jnp.bfloat16)


def levels(rng, dims, pieces, smallest, top_value):
    def one(position, shards_of):
        draws = jax.random.uniform(jax.random.fold_in(jax.random.fold_in(rng, 6), position), (shards_of,), jnp.float32, smallest / len(pieces), top_value / len(pieces))
        return jnp.repeat(jnp.exp(draws), dims[position] // shards_of).reshape((-1,) + (1,) * (len(dims) - position - 1))

    level = one(*pieces[0])
    for cut in pieces[1:]:
        level = level * one(*cut)
    return level


def gaussian(key, dims, spread, bound, shards=(), held_as=jnp.bfloat16):
    factor_of = levels(key, dims, shards, -0.22, 0.18) if shards else 1.0
    result = jax.random.normal(key, dims, jnp.float32) * spread * factor_of
    return jnp.minimum(jnp.maximum(result, -bound), bound).astype(held_as)


def setup_inputs(seed: int = 0) -> dict:
    key_of = jax.random.split(jax.random.key(seed), 7)
    return {
        "queries": draw_queries(jax.random.fold_in(key_of[6], 71), 0),
        "latent": draw_latent(jax.random.fold_in(key_of[6], 71), 0),
        "block_of": jax.random.permutation(key_of[2], BLOCKS).astype(jnp.int32),
        "key_up": gaussian(key_of[3], (HEADS, NOPE, LATENT), NOPE ** -0.5, 0.5, ((0, 8),)),
        "value_up": gaussian(key_of[4], (HEADS, LATENT, VHEAD), LATENT ** -0.5, 0.25, ((0, 8),)),
        "out_grad": gaussian(key_of[5], (TOKENS, HEADS * VHEAD), 1.0, 6.0, ((0, 4), (1, 8))),
    }


def reference(queries, latent, block_of, key_up, value_up, out_grad):
    rows = jnp.arange(TOKENS, dtype=jnp.int32)
    positions = jnp.take(block_of, (rows // BLK).astype(jnp.int32)).astype(jnp.int32) * BLK + rows % BLK
    visible = positions[None, :] <= positions[:, None]
    score_scale = 1.0 / math.sqrt(NOPE + ROPE)
    latent_part = latent[:, :LATENT]
    query_heads = jnp.transpose(queries.reshape(TOKENS, HEADS, NOPE + ROPE), (1, 0, 2))
    grad_heads = jnp.transpose(out_grad.reshape(TOKENS, HEADS, VHEAD), (1, 0, 2))

    def one_head(total, inputs):
        query_one, up_key, up_value, grad_one = inputs
        q_latent = jnp.dot(query_one[:, :NOPE], up_key, preferred_element_type=jnp.float32).astype(jnp.bfloat16)
        q_joined = jnp.concatenate([q_latent, query_one[:, NOPE:]], axis=1)
        scores = jnp.dot(q_joined, latent.T, preferred_element_type=jnp.float32) * score_scale
        scores = jnp.where(visible, scores, -1e+30)
        row_max = lax.optimization_barrier(jnp.max(scores, axis=1, keepdims=True))
        expo = jnp.exp(scores - row_max)
        probs = expo / lax.optimization_barrier(jnp.sum(expo, axis=1, keepdims=True))
        probs_low = probs.astype(jnp.bfloat16)
        out_latent = jnp.dot(probs_low, latent_part, preferred_element_type=jnp.float32).astype(jnp.bfloat16)
        attended = jnp.dot(out_latent, up_value, preferred_element_type=jnp.float32).astype(jnp.bfloat16)
        grad_latent = jnp.dot(grad_one, up_value.T, preferred_element_type=jnp.float32).astype(jnp.bfloat16)
        grad_probs = jnp.dot(grad_latent, latent_part.T, preferred_element_type=jnp.float32)
        delta = lax.optimization_barrier(jnp.sum(probs * grad_probs, axis=1, keepdims=True))
        grad_scores = (probs * (grad_probs - delta) * score_scale).astype(jnp.bfloat16)
        grad_joined = jnp.dot(grad_scores, latent, preferred_element_type=jnp.float32)
        grad_nope = jnp.dot(grad_joined[:, :LATENT].astype(jnp.bfloat16), up_key.T, preferred_element_type=jnp.float32).astype(jnp.bfloat16)
        grad_query = jnp.concatenate([grad_nope, grad_joined[:, LATENT:].astype(jnp.bfloat16)], axis=1)
        grad_keys = jnp.dot(grad_scores.T, q_joined, preferred_element_type=jnp.float32)
        value_part = jnp.dot(probs_low.T, grad_latent, preferred_element_type=jnp.float32)
        grad_keys = grad_keys + jnp.pad(value_part, ((0, 0), (0, ROPE)))
        return (total + grad_keys, (attended, grad_query))
    start = jnp.zeros((TOKENS, LATENT + ROPE), jnp.float32)
    latent_grad, (attended, query_grad) = lax.scan(one_head, start, (query_heads, key_up, value_up, grad_heads))
    attended = jnp.transpose(attended, (1, 0, 2)).reshape(TOKENS, HEADS * VHEAD)
    query_grad = jnp.transpose(query_grad, (1, 0, 2)).reshape(TOKENS, HEADS * (NOPE + ROPE))
    return (attended, query_grad, latent_grad)
```

```python
import functools
import math

import jax
import jax.numpy as jnp
from jax import lax
from jax.experimental import pallas as pl
from jax.experimental.pallas import tpu as pltpu
from jax.sharding import PartitionSpec as P

BF = jnp.bfloat16
F32 = jnp.float32
VM = pl.BlockSpec(memory_space=pltpu.VMEM)
SM = pl.BlockSpec(memory_space=pltpu.SMEM)


def dot(a, b, da, db):
    return lax.dot_general(a, b, (((da,), (db,)), ((), ())), preferred_element_type=F32)


def prepare_kernel(heads, nope, q_ref, ku_ref, vu_ref, og_ref, qj_ref, gl_ref, qjt_ref, glt_ref):
    rows = q_ref.shape[0]
    qw = q_ref.shape[1] // heads
    latent = ku_ref.shape[2]
    vw = vu_ref.shape[2]
    for h in range(heads):
        here = pl.ds(h * rows, rows)
        qh = q_ref[:, h * qw : (h + 1) * qw]
        ql = dot(qh[:, :nope], ku_ref[h], 1, 0).astype(BF)
        qr = qh[:, nope:]
        qj_ref[here, :latent] = ql
        qj_ref[here, latent:] = qr
        qjt_ref[:latent, here] = ql.T
        qjt_ref[latent:, here] = qr.T
        gl = dot(og_ref[:, h * vw : (h + 1) * vw], vu_ref[h], 1, 1).astype(BF)
        gl_ref[here, :] = gl
        glt_ref[:, here] = gl.T


def attend_kernel(
    ctx, scale, partner_of, heads, latent,
    blk_ref, qj_ref, gl_ref, qjt_ref, glt_ref, own_ref, *rest
):
    n = ctx
    mine = rest[: n - 1]
    other = rest[n - 1 : 2 * n - 2]
    lt_ref, pr_ref, gs_ref, keep_ref, send_ref, gt_ref = rest[2 * n - 2 :]
    me = lax.axis_index("ctx")
    core = lax.rem(lax.axis_index("head"), 2)
    rows = own_ref.shape[1]
    joined = own_ref.shape[0]
    half = joined // 2
    total = rows * n
    per = blk_ref.shape[0] // n
    blk = rows // per
    m0 = pl.multiple_of(core * half, 16)
    o0 = pl.multiple_of((1 - core) * half, 16)
    lt_ref[:, :rows] = own_ref[...]
    for k in range(1, n):
        cols = pl.ds(k * rows, rows)
        lt_ref[pl.ds(m0, half), cols] = mine[k - 1][...]
        lt_ref[pl.ds(o0, half), cols] = other[k - 1][...]

    def positions(owner, index):
        base = jnp.zeros(index.shape, jnp.int32)
        for j in range(per):
            base = jnp.where(index // blk == j, blk_ref[owner * per + j] * blk, base)
        return base + index % blk

    qpos = positions(me, lax.broadcasted_iota(jnp.int32, (rows, rows), 0))
    qpos = jnp.concatenate([qpos] * heads, axis=0)
    lane = lax.broadcasted_iota(jnp.int32, (1, rows), 1)
    visible = jnp.concatenate(
        [positions(partner_of(me, k), lane) <= qpos for k in range(n)], axis=1
    )
    s = dot(qj_ref[...], lt_ref[...], 1, 0) * scale
    s = jnp.where(visible, s, -1e30)
    e = jnp.exp(s - jnp.max(s, axis=1, keepdims=True))
    p = e / jnp.sum(e, axis=1, keepdims=True)
    p_low = p.astype(BF)
    pr_ref[...] = p_low
    gp = dot(gl_ref[...], lt_ref[:latent, :], 1, 0)
    delta = jnp.sum(p * gp, axis=1, keepdims=True)
    gs = (p * (gp - delta) * scale).astype(BF)
    gs_ref[...] = gs
    gt_ref[...] = dot(qjt_ref[...], gs, 1, 0)
    gt_ref[:latent, :] += dot(glt_ref[...], p_low, 1, 0)
    for k in range(n):
        cols = pl.ds(k * rows, rows)
        keep_ref[k] = gt_ref[pl.ds(m0, half), cols]
        send_ref[k] = gt_ref[pl.ds(o0, half), cols].astype(BF)


def finish_kernel(heads, nope, pr_ref, gs_ref, lt_ref, ku_ref, vu_ref, at_ref, qg_ref):
    rows = at_ref.shape[0]
    latent = ku_ref.shape[2]
    vw = vu_ref.shape[2]
    qw = qg_ref.shape[1] // heads
    ol = dot(pr_ref[...], lt_ref[:latent, :], 1, 1).astype(BF)
    gj = dot(gs_ref[...], lt_ref[...], 1, 1).astype(BF)
    for h in range(heads):
        here = slice(h * rows, (h + 1) * rows)
        at_ref[:, h * vw : (h + 1) * vw] = dot(ol[here], vu_ref[h], 1, 0).astype(BF)
        gn = dot(gj[here, :latent], ku_ref[h], 1, 1).astype(BF)
        qg_ref[:, h * qw : h * qw + nope] = gn
        qg_ref[:, h * qw + nope : (h + 1) * qw] = gj[here, latent:]


def call(kernel, outs, ins, scratch=(), flops=0, nbytes=0):
    return pl.pallas_call(
        kernel,
        out_shape=[jax.ShapeDtypeStruct(s, d) for s, d in outs],
        in_specs=ins,
        out_specs=[VM] * len(outs),
        scratch_shapes=list(scratch),
        cost_estimate=pl.CostEstimate(flops=flops, bytes_accessed=nbytes, transcendentals=0),
        compiler_params=pltpu.CompilerParams(vmem_limit_bytes=48 << 20),
    )


def partner(n, k):
    if n & (n - 1) == 0:
        return lambda i: i ^ k
    return lambda i: (i + k) % n


def digits(n):
    out = []
    f = 2
    while n > 1:
        while n % f == 0:
            out.append(f)
            n //= f
        f += 1
    return out


def on_device(ctx, head, queries, latent, block_of, key_up, value_up, out_grad):
    rows = queries.shape[0]
    heads, nope, width = key_up.shape
    joined = latent.shape[1]
    vw = value_up.shape[2]
    qw = queries.shape[1] // heads
    scale = 1.0 / math.sqrt(qw)
    half = joined // 2
    total = rows * ctx
    hr = heads * rows
    core = lax.rem(lax.axis_index("head"), 2)

    def ctx_send(x, k):
        return lax.ppermute(x, "ctx", [(i, partner(ctx, k)(i)) for i in range(ctx)])

    def ctx_fetch(x, k):
        return lax.ppermute(x, "ctx", [(partner(ctx, k)(i), i) for i in range(ctx)])

    def swap(x):
        return lax.ppermute(x, "head", [(i, i ^ 1) for i in range(head)])

    lt_own = latent.T
    piece = jnp.where(core == 0, lt_own[:half], lt_own[half:])
    order = sorted(range(1, ctx), key=lambda k: -bin(k).count("1"))
    mine = {k: ctx_fetch(piece, k) for k in order}
    other = {k: swap(mine[k]) for k in order}

    qj, gl, qjt, glt = call(
        functools.partial(prepare_kernel, heads, nope),
        [((hr, joined), BF), ((hr, width), BF), ((joined, hr), BF), ((width, hr), BF)],
        [VM] * 4,
        flops=4 * hr * nope * width,
        nbytes=2 * hr * joined * 6,
    )(queries, key_up, value_up, out_grad)

    partner_of = (lambda i, k: i ^ k) if ctx & (ctx - 1) == 0 else (lambda i, k: lax.rem(i + k, ctx))
    lt, pr, gs, keep, send = call(
        functools.partial(attend_kernel, ctx, scale, partner_of, heads, width),
        [
            ((joined, total), BF),
            ((hr, total), BF),
            ((hr, total), BF),
            ((ctx, half, rows), F32),
            ((ctx, half, rows), BF),
        ],
        [SM] + [VM] * (3 + 2 * ctx),
        [pltpu.VMEM((joined, total), F32)],
        flops=8 * hr * joined * total,
        nbytes=2 * joined * total,
    )(
        block_of, qj, gl, qjt, glt, lt_own,
        *[mine[k] for k in range(1, ctx)], *[other[k] for k in range(1, ctx)],
    )
    chip = keep + swap(send).astype(F32)
    got = {k: ctx_send(chip[k].astype(BF), k) for k in order}
    attended, query_grad = call(
        functools.partial(finish_kernel, heads, nope),
        [((rows, heads * vw), BF), ((rows, heads * qw), BF)],
        [VM] * 5,
        flops=4 * hr * joined * total,
        nbytes=2 * joined * total,
    )(pr, gs, lt, key_up, value_up)

    acc = chip[0]
    for k in order:
        acc = acc + got[k].astype(F32)
    step = 2
    for f in digits(head // 2):
        part = acc.astype(BF)
        sent = []
        for j in range(1, f):
            pairs = []
            for i in range(head):
                d = (i // step) % f
                pairs.append((i, i + ((d + j) % f - d) * step))
            sent.append(lax.ppermute(part, "head", pairs))
        if f == 2:
            acc = part.astype(F32) + sent[0].astype(F32)
        else:
            terms = [part] + sent
            mydigit = lax.rem(lax.axis_index("head") // step, f)
            acc = jnp.zeros(part.shape, F32)
            for s in range(f):
                t = terms[0]
                for j in range(1, f):
                    t = jnp.where(lax.rem(mydigit - j + f, f) == s, terms[j], t)
                t = jnp.where(mydigit == s, terms[0], t)
                acc = acc + t.astype(F32)
        step *= f
    theirs = swap(acc)
    low = jnp.where(core == 0, acc, theirs)
    high = jnp.where(core == 0, theirs, acc)
    return attended, query_grad, jnp.concatenate([low, high], axis=0).T


def solution(mesh):
    ctx, head = mesh.shape["ctx"], mesh.shape["head"]
    return jax.shard_map(
        functools.partial(on_device, ctx, head),
        mesh=mesh,
        in_specs=(
            P("ctx", "head"),
            P("ctx", None),
            P(),
            P("head", None, None),
            P("head", None, None),
            P("ctx", "head"),
        ),
        out_specs=(P("ctx", "head"), P("ctx", "head"), P("ctx", None)),
        check_vma=False,
    )
```

```python
import functools
import math

import jax
import jax.numpy as jnp
from jax import lax
from jax.experimental import pallas as pl
from jax.experimental.pallas import tpu as pltpu
from jax.sharding import PartitionSpec as P


BF = jnp.bfloat16
F32 = jnp.float32
VM = pl.BlockSpec(memory_space=pltpu.VMEM)
SM = pl.BlockSpec(memory_space=pltpu.SMEM)
HB = pl.BlockSpec(memory_space=pltpu.HBM)


def dot(a, b, da, db):
    return lax.dot_general(a, b, (((da,), (db,)), ((), ())), preferred_element_type=F32)


def prepare_kernel(
    heads, nope, q_hbm, ku_hbm, vu_hbm, og_hbm, qj_ref, gl_ref, qjt_ref, glt_ref,
    q_ref, ku_ref, vu_ref, og_ref, sems,
):
    copies = [
        pltpu.make_async_copy(src, dst, sems.at[i])
        for i, (src, dst) in enumerate(
            ((q_hbm, q_ref), (ku_hbm, ku_ref), (og_hbm, og_ref), (vu_hbm, vu_ref))
        )
    ]
    for c in copies:
        c.start()
    for c in copies:
        c.wait()
    rows = q_ref.shape[0]
    qw = q_ref.shape[1] // heads
    latent = ku_ref.shape[2]
    vw = vu_ref.shape[2]
    for h in range(heads):
        here = pl.ds(h * rows, rows)
        qh = q_ref[:, h * qw : (h + 1) * qw]
        ql = dot(qh[:, :nope], ku_ref[h], 1, 0).astype(BF)
        qr = qh[:, nope:]
        qj_ref[here, :latent] = ql
        qj_ref[here, latent:] = qr
        qjt_ref[:latent, here] = ql.T
        qjt_ref[latent:, here] = qr.T
        gl = dot(og_ref[:, h * vw : (h + 1) * vw], vu_ref[h], 1, 1).astype(BF)
        gl_ref[here, :] = gl
        glt_ref[:, here] = gl.T


def attend_kernel(
    ctx, scale, partner_of, heads, latent,
    blk_ref, qj_ref, gl_ref, qjt_ref, glt_ref, own_ref, *rest
):
    n = ctx
    mine = rest[: n - 1]
    other = rest[n - 1 : 2 * n - 2]
    lt_ref, pr_ref, gs_ref, keep_ref, send_ref, gt_ref = rest[2 * n - 2 :]
    me = lax.axis_index("ctx")
    core = lax.rem(lax.axis_index("head"), 2)
    rows = own_ref.shape[1]
    joined = own_ref.shape[0]
    half = joined // 2
    per = blk_ref.shape[0] // n
    blk = rows // per
    m0 = pl.multiple_of(core * half, 16)
    o0 = pl.multiple_of((1 - core) * half, 16)
    lt_ref[:, :rows] = own_ref[...]
    for k in range(1, n):
        cols = pl.ds(k * rows, rows)
        lt_ref[pl.ds(m0, half), cols] = mine[k - 1][...]
        lt_ref[pl.ds(o0, half), cols] = other[k - 1][...]

    def positions(owner, index):
        base = jnp.zeros(index.shape, jnp.int32)
        for j in range(per):
            base = jnp.where(index // blk == j, blk_ref[owner * per + j] * blk, base)
        return base + index % blk

    qpos = positions(me, lax.broadcasted_iota(jnp.int32, (rows, rows), 0))
    qpos = jnp.concatenate([qpos] * heads, axis=0)
    lane = lax.broadcasted_iota(jnp.int32, (1, rows), 1)
    visible = jnp.concatenate(
        [positions(partner_of(me, k), lane) <= qpos for k in range(n)], axis=1
    )
    s = dot(qj_ref[...], lt_ref[...], 1, 0) * scale
    s = jnp.where(visible, s, -1e30)
    e = jnp.exp(s - jnp.max(s, axis=1, keepdims=True))
    p = e / jnp.sum(e, axis=1, keepdims=True)
    p_low = p.astype(BF)
    pr_ref[...] = p_low
    gp = dot(gl_ref[...], lt_ref[:latent, :], 1, 0)
    delta = jnp.sum(p * gp, axis=1, keepdims=True)
    gs = (p * (gp - delta) * scale).astype(BF)
    gs_ref[...] = gs
    gt_ref[...] = dot(qjt_ref[...], gs, 1, 0)
    gt_ref[:latent, :] += dot(glt_ref[...], p_low, 1, 0)
    for k in range(n):
        cols = pl.ds(k * rows, rows)
        keep_ref[k] = gt_ref[pl.ds(m0, half), cols]
        send_ref[k] = gt_ref[pl.ds(o0, half), cols].astype(BF)


def finish_kernel(heads, nope, pr_ref, gs_ref, lt_ref, ku_ref, vu_ref, at_ref, qg_ref):
    rows = at_ref.shape[0]
    latent = ku_ref.shape[2]
    vw = vu_ref.shape[2]
    qw = qg_ref.shape[1] // heads
    ol = dot(pr_ref[...], lt_ref[:latent, :], 1, 1).astype(BF)
    gj = dot(gs_ref[...], lt_ref[...], 1, 1).astype(BF)
    for h in range(heads):
        here = slice(h * rows, (h + 1) * rows)
        at_ref[:, h * vw : (h + 1) * vw] = dot(ol[here], vu_ref[h], 1, 0).astype(BF)
        gn = dot(gj[here, :latent], ku_ref[h], 1, 1).astype(BF)
        qg_ref[:, h * qw : h * qw + nope] = gn
        qg_ref[:, h * qw + nope : (h + 1) * qw] = gj[here, latent:]


def call(kernel, outs, ins, scratch=(), flops=0, nbytes=0):
    return pl.pallas_call(
        kernel,
        out_shape=[jax.ShapeDtypeStruct(s, d) for s, d in outs],
        in_specs=ins,
        out_specs=[VM] * len(outs),
        scratch_shapes=list(scratch),
        cost_estimate=pl.CostEstimate(flops=flops, bytes_accessed=nbytes, transcendentals=0),
        compiler_params=pltpu.CompilerParams(vmem_limit_bytes=48 << 20),
    )


def partner(n, k):
    if n & (n - 1) == 0:
        return lambda i: i ^ k
    return lambda i: (i + k) % n


def digits(n):
    out = []
    f = 2
    while n > 1:
        while n % f == 0:
            out.append(f)
            n //= f
        f += 1
    return out


def attention(ctx, head, queries, latent, block_of, key_up, value_up, out_grad):
    rows = queries.shape[0]
    heads, nope, width = key_up.shape
    joined = latent.shape[1]
    vw = value_up.shape[2]
    qw = queries.shape[1] // heads
    scale = 1.0 / math.sqrt(qw)
    half = joined // 2
    total = rows * ctx
    hr = heads * rows
    core = lax.rem(lax.axis_index("head"), 2)

    def ctx_send(x, k):
        return lax.ppermute(x, "ctx", [(i, partner(ctx, k)(i)) for i in range(ctx)])

    def ctx_fetch(x, k):
        return lax.ppermute(x, "ctx", [(partner(ctx, k)(i), i) for i in range(ctx)])

    def swap(x):
        return lax.ppermute(x, "head", [(i, i ^ 1) for i in range(head)])

    lt_own = latent.T
    piece = jnp.where(core == 0, lt_own[:half], lt_own[half:])
    order = sorted(range(1, ctx), key=lambda k: -bin(k).count("1"))
    mine = {}
    for k in order:
        mine[k] = ctx_fetch(piece, k)
    other = {k: swap(mine[k]) for k in order}

    def hbm(x):
        return pltpu.with_memory_space_constraint(x, pltpu.HBM)

    qj, gl, qjt, glt = call(
      functools.partial(prepare_kernel, heads, nope),
      [((hr, joined), BF), ((hr, width), BF), ((joined, hr), BF), ((width, hr), BF)],
      [HB] * 4,
      [
          pltpu.VMEM(queries.shape, BF),
          pltpu.VMEM(key_up.shape, BF),
          pltpu.VMEM(value_up.shape, BF),
          pltpu.VMEM(out_grad.shape, BF),
          pltpu.SemaphoreType.DMA((4,)),
      ],
      flops=4 * hr * nope * width,
      nbytes=2 * hr * joined * 6,
    )(hbm(queries), hbm(key_up), hbm(value_up), hbm(out_grad))

    partner_of = (lambda i, k: i ^ k) if ctx & (ctx - 1) == 0 else (lambda i, k: lax.rem(i + k, ctx))
    lt, pr, gs, keep, send = call(
        functools.partial(attend_kernel, ctx, scale, partner_of, heads, width),
        [
            ((joined, total), BF),
            ((hr, total), BF),
            ((hr, total), BF),
            ((ctx, half, rows), F32),
            ((ctx, half, rows), BF),
        ],
        [SM] + [VM] * (3 + 2 * ctx),
        [pltpu.VMEM((joined, total), F32)],
        flops=8 * hr * joined * total,
        nbytes=2 * joined * total,
    )(
        block_of, qj, gl, qjt, glt, lt_own,
        *[mine[k] for k in range(1, ctx)], *[other[k] for k in range(1, ctx)],
    )
    chip = keep + swap(send).astype(F32)
    got = {k: ctx_send(chip[k].astype(BF), k) for k in order}
    attended, query_grad = call(
      functools.partial(finish_kernel, heads, nope),
      [((rows, heads * vw), BF), ((rows, heads * qw), BF)],
      [VM] * 5,
      flops=4 * hr * joined * total,
      nbytes=2 * joined * total,
    )(pr, gs, lt, key_up, value_up)

    acc = chip[0]
    for k in order:
        acc = acc + got[k].astype(F32)
    step = 2
    for f in digits(head // 2):
        part = acc.astype(BF)
        sent = []
        for j in range(1, f):
            pairs = []
            for i in range(head):
                d = (i // step) % f
                pairs.append((i, i + ((d + j) % f - d) * step))
            sent.append(lax.ppermute(part, "head", pairs))
        if f == 2:
            acc = part.astype(F32) + sent[0].astype(F32)
        else:
            terms = [part] + sent
            mydigit = lax.rem(lax.axis_index("head") // step, f)
            acc = jnp.zeros(part.shape, F32)
            for s in range(f):
                t = terms[0]
                for j in range(1, f):
                    t = jnp.where(lax.rem(mydigit - j + f, f) == s, terms[j], t)
                t = jnp.where(mydigit == s, terms[0], t)
                acc = acc + t.astype(F32)
        step *= f
    theirs = swap(acc)
    low = jnp.where(core == 0, acc, theirs)
    high = jnp.where(core == 0, theirs, acc)
    return attended, query_grad, jnp.concatenate([low, high], axis=0).T


def solution(mesh):
    ctx, head = mesh.shape["ctx"], mesh.shape["head"]
    return jax.shard_map(
        functools.partial(attention, ctx, head),
        mesh=mesh,
        in_specs=(
            P("ctx", "head"),
            P("ctx", None),
            P(),
            P("head", None, None),
            P("head", None, None),
            P("ctx", "head"),
        ),
        out_specs=(P("ctx", "head"), P("ctx", "head"), P("ctx", None)),
        check_vma=False,
    )
```
